32 devices in a mesh: expert: 16 (over z, x, core), tensor: 2 (over y).
Axes of the slice: x: 2, y: 2, z: 4, core: 2. Of those that a mesh axis runs over, the one named last changes fastest.
Arguments:
- tokens: bfloat16 [256, 7168], P('expert'), may hold values from -6 to 6
- routes: int32 [256, 8], P('expert'), may hold values from 0 to 15, all different within a row; in each aligned block of 16 rows (0 to 15, 16 to 31, ...) at most 8 rows name the same one
- route_logits: float32 [256, 8], P('expert'), may hold values from -8 to 8
- gate_weight: bfloat16 [16, 7168, 1024], P('expert', 'tensor'), may hold values from -0.0625 to 0.0625
- up_weight: bfloat16 [16, 7168, 1024], P('expert', 'tensor'), may hold values from -0.0625 to 0.0625
- down_weight: bfloat16 [16, 7168, 1024], P('expert', 'tensor'), may hold values from -0.1875 to 0.1875
Outputs:
- mixed: bfloat16 [256, 7168], P('expert', 'tensor')
The draws below stay inside these ranges and needn't reach their ends.
Inputs may be any that keep to these rules, and one draw needn't show every extreme that they name: `routes`: each row names 8 different experts. In each aligned block of 16 rows (the rows of one index of expert) no expert is named by more than 8 rows, a bound that some block reaches.
All inputs are finite; a program needn't handle non-finite values.
Results may differ from the reference program's by a relative error of at most 0.0066.
Values may be sent and summed in bfloat16 or wider, within the bound.
A program may use at most 64 MiB of HBM per device.

```python
import math
import jax
import jax.numpy as jnp
import numpy as np
from jax import lax

D = 7168
F = 1024
TOP = 8
TOK_DEV = 16
EXPERTS = 16
CAP = 8
TOKENS = 256


def block_scale(rng, dims, shards, low, top_value):
    level = 1.0
    for axis_at, shards_of in shards:
        steps = jax.random.uniform(jax.random.fold_in(jax.random.fold_in(rng, 6), axis_at), (shards_of,), jnp.float32, low / len(shards), top_value / len(shards))
        level = level * jnp.repeat(jnp.exp(steps), dims[axis_at] // shards_of).reshape((-1,) + (1,) * (len(dims) - 1 - axis_at))
    return level


def deal_out(key, own, number, rows, number_of, top, limit, skew):
    sequence = jax.random.permutation(key, number_of)
    crowded, usual = portions_of(number_of, rows * top, limit, skew, True), portions_of(number_of, rows * top, limit, skew, False)
    places = jnp.arange(number_of)

    def named(tallies, offset_by):
        used = int((tallies > 0).sum())
        fixed = max(1, used // 4)
        shifted = fixed + (places - fixed + offset_by * (used - fixed)) % max(1, number_of - fixed)
        return jnp.zeros((number_of,), jnp.int32).at[sequence[jnp.where(places < fixed, places, shifted)]].set(jnp.asarray(tallies, jnp.int32))

    tallies = jnp.where(number % 4 == 0, named(crowded, number // 4), named(usual, number - number // 4 - 1))
    mixed = jax.random.permutation(jax.random.fold_in(own, 3), number_of)
    donor, receiver = mixed[0:number_of // 2 * 2:2], mixed[1:number_of // 2 * 2:2]
    slack = jnp.minimum(tallies[donor] - 1, limit - tallies[receiver]) // 2
    slack = jnp.where((donor == sequence[0]) | (receiver == sequence[0]) | (tallies[receiver] == 0), 0, jnp.maximum(slack, 0))
    shifted = jax.random.randint(jax.random.fold_in(own, 4), (number_of // 2,), 0, 1 << 20) % (slack + 1)
    tallies = tallies.at[donor].add(-shifted).at[receiver].add(shifted)
    items = jnp.searchsorted(jnp.cumsum(tallies), jnp.arange(rows * top), side="right").astype(jnp.int32)
    listing = items.reshape(top, rows).T
    listing = listing[jax.random.permutation(jax.random.fold_in(own, 1), rows)]
    offset_by = jax.random.randint(jax.random.fold_in(own, 2), (rows, 1), 0, top)
    return jnp.take_along_axis(listing, (jnp.arange(top)[None, :] + offset_by) % top, axis=1)


def portions_of(count, total, limit, slope, full):
    loads = [(1 << 20) // math.isqrt(grade ** slope) + 1 for grade in range(1, count + 1)]
    largest = limit if full else min(limit, max(-(-total // count), total * loads[0] // sum(loads)))
    least = 1 if total - largest >= count - 1 else 0
    holding, surplus = [largest] + [least] * (count - 1), total - largest - least * (count - 1)
    while surplus > 0:
        free = [i for i in range(1, count) if holding[i] < largest] or [i for i in range(1, count) if holding[i] < limit]
        whole, remaining = sum([loads[i] for i in free]), surplus
        for i in free:
            more = min(limit - holding[i], max(1, remaining * loads[i] // whole), surplus)
            holding[i] = holding[i] + more
            surplus = surplus - more
    return np.array(holding)


def noise(rng, extent, deviation, limit, pieces=(), kind=jnp.bfloat16):
    drawn = deviation * jax.random.normal(rng, extent, jnp.float32)
    if pieces:
        drawn = drawn * block_scale(rng, extent, pieces, -0.22, 0.18)
    return jnp.clip(drawn, -limit, limit).astype(kind)


def setup_inputs(seed: int = 0) -> dict:
    seeds = jax.random.split(jax.random.key(seed), 7)
    tokens = noise(seeds[0], (TOKENS, D), 1.0, 6.0, ((0, 16),))
    routes_keys = jax.random.split(jax.random.fold_in(seeds[1], 1), TOKENS // TOK_DEV)
    routes_turns = jax.random.permutation(jax.random.fold_in(seeds[1], 3), TOKENS // TOK_DEV)
    routes = jax.vmap(lambda own, number: deal_out(jax.random.fold_in(seeds[1], 2), own, number, TOK_DEV, EXPERTS, TOP, CAP, 2))(routes_keys, routes_turns).reshape((TOKENS, TOP))
    route_logits = noise(seeds[2], (TOKENS, TOP), 2.0, 8.0, ((0, 16),), jnp.float32)
    gate_weight = noise(seeds[3], (EXPERTS, D, F), D ** -0.5, 0.0625, ((0, 16), (1, 2)))
    up_weight = noise(seeds[4], (EXPERTS, D, F), D ** -0.5, 0.0625, ((0, 16), (1, 2)))
    down_weight = noise(seeds[5], (EXPERTS, D, F), F ** -0.5, 0.1875, ((0, 16), (1, 2)))
    return {"tokens": tokens, "routes": routes, "route_logits": route_logits, "gate_weight": gate_weight, "up_weight": up_weight, "down_weight": down_weight}


routed_scale = 2.5


def reference(tokens, routes, route_logits, gate_weight, up_weight, down_weight):
    scores = jax.nn.sigmoid(route_logits)
    weights = routed_scale * scores / jnp.sum(scores, axis=1, keepdims=True)
    block_count = TOKENS // TOK_DEV
    flat_routes = routes.reshape(block_count, TOK_DEV * TOP).astype(jnp.int32)
    one_hot = (flat_routes[:, :, None] == jnp.arange(EXPERTS, dtype=jnp.int32)[None, None, :]).astype(jnp.int32)
    earlier = jnp.cumsum(one_hot, axis=1) - one_hot
    position = jnp.sum(earlier * one_hot, axis=2).astype(jnp.int32)
    block_ids = jnp.broadcast_to(jnp.arange(block_count, dtype=jnp.int32)[:, None], flat_routes.shape).astype(jnp.int32)
    token_ids = (block_ids * TOK_DEV + jnp.arange(TOK_DEV * TOP, dtype=jnp.int32)[None, :] // TOP).astype(jnp.int32)
    table = jnp.zeros((EXPERTS, block_count, CAP), jnp.int32).at[flat_routes, block_ids, position].set(token_ids)
    portions = jnp.zeros((EXPERTS, block_count, CAP), jnp.float32).at[flat_routes, block_ids, position].set(
        weights.reshape(block_count, TOK_DEV * TOP).astype(jnp.float32))

    def expert_step(accumulated, expert_item):
        gate_w, up_w, down_w, rows_at, portion = expert_item
        row_index = rows_at.reshape(-1).astype(jnp.int32)
        picked = tokens[row_index]
        gate_value = jnp.dot(picked, gate_w, preferred_element_type=jnp.float32)
        up_value = jnp.dot(picked, up_w, preferred_element_type=jnp.float32)
        hidden = (jax.nn.silu(gate_value) * up_value).astype(jnp.bfloat16)
        output = jnp.dot(hidden, down_w.T, preferred_element_type=jnp.float32)
        accumulated = accumulated.at[row_index].add(portion.reshape(-1)[:, None] * output)
        return accumulated, None

    start = jnp.zeros((TOKENS, D), jnp.float32)
    accumulated, _ = lax.scan(expert_step, start, (gate_weight, up_weight, down_weight, table, portions))
    return accumulated.astype(jnp.bfloat16)
```

```python
import functools

import jax
import jax.numpy as jnp
from jax import lax
from jax.experimental import pallas as pl
from jax.experimental.pallas import tpu as pltpu
from jax.sharding import PartitionSpec as P

routed_scale = 2.5
MESH = pl.DeviceIdType.MESH
BF = jnp.bfloat16
F32 = jnp.float32


def kernel(
    dims,
    tokens_ref,
    routes_ref,
    logits_ref,
    gate_hbm,
    up_hbm,
    down_hbm,
    out_ref,
    G,
    gw,
    uw,
    dw,
    X,
    ysend,
    yrecv,
    hid,
    dense,
    crecv,
    s1,
    xrecv,
    s2,
    zrecv,
    wsem,
    tsem,
    grecv,
    gz,
    gx,
    gc,
    ys,
    yr,
    hs,
    hr,
    cs,
    cr,
    xs,
    xr,
    zs,
    zr,
):
    E, T, A, B, tok, cap, top, Dl, F, lanes, nd, dc, fc, nj, pieces = dims
    R, NT, FT = E * cap, E * tok, F // T
    e = lax.axis_index("expert")
    t = lax.axis_index("tensor")
    c = lax.rem(e, 2)
    b = lax.rem(e // 2, B)
    a = e // (2 * B)

    def around(v, i, n):
        return lax.rem(v + i, n)

    def slot_of(ai, bi, ci):
        return (ai * B + bi) * 2 + ci

    def dev(ai, bi, ci):
        return (slot_of(ai, bi, ci), t)

    half = Dl // 256 * 128
    spans = ((0, half), (half, Dl - half))
    barrier = pltpu.get_barrier_semaphore()
    partners = [dev(around(a, i, A), b, c) for i in range(1, A)]
    partners += [dev(a, around(b, k, B), c) for k in range(1, B)]
    partners += [dev(a, b, 1 - c)]
    partners += [(e, around(t, p, T)) for p in range(1, T)]
    for partner in partners:
        pl.semaphore_signal(barrier, inc=1, device_id=partner, device_id_type=MESH)

    token_copies = []
    for h, (first, width) in enumerate(spans):
        copy = pltpu.make_async_copy(
            tokens_ref.at[:, pl.ds(pl.multiple_of(t * Dl + first, 128), width)],
            G.at[pl.ds(pl.multiple_of(e * tok, tok), tok), pl.ds(first, width)],
            tsem.at[h],
        )
        copy.start()
        token_copies.append(copy)

    scores = jax.nn.sigmoid(logits_ref[...])
    weights = routed_scale * scores / jnp.sum(scores, axis=0, keepdims=True)
    routes = routes_ref[...]
    lane = lax.broadcasted_iota(jnp.int32, (lanes, tok), 0)
    table = jnp.zeros((lanes, tok), F32)
    for k in range(top):
        table += jnp.where(lane == routes[k : k + 1], weights[k : k + 1], 0.0)
    high = table.astype(BF)
    low = (table - high.astype(F32)).astype(BF)
    nt = (((1,), (1,)), ((), ()))
    unit = lax.broadcasted_iota(jnp.int32, (tok, tok), 0) == lax.broadcasted_iota(jnp.int32, (tok, tok), 1)
    unit = jnp.where(unit, 1.0, 0.0).astype(BF)
    high = lax.dot_general(unit, high, nt, preferred_element_type=F32).astype(BF)
    low = lax.dot_general(unit, low, nt, preferred_element_type=F32).astype(BF)

    def block(slot):
        return pl.ds(pl.multiple_of(slot * tok, tok), tok)

    G[block(e), pl.ds(Dl, lanes)] = high
    G[block(e), pl.ds(Dl + lanes, lanes)] = low
    pl.semaphore_wait(barrier, len(partners))
    for copy in token_copies:
        copy.wait()

    step_in, step_out = Dl // pieces, Dl // pieces
    weight_copies = []
    for which, (src, dst) in enumerate(((gate_hbm, gw), (up_hbm, uw), (down_hbm, dw))):
        for p in range(pieces):
            rows = pl.ds(p * step_in, step_in)
            copy = pltpu.make_async_copy(src.at[0, rows], dst.at[rows], wsem.at[which, p])
            copy.start()
            weight_copies.append(copy)

    parts = ((0, half), (half, Dl - half + 2 * lanes))

    def gcopy(slot, h, target, sem):
        cols = pl.ds(*parts[h])
        return pltpu.make_async_remote_copy(
            src_ref=G.at[block(slot), cols],
            dst_ref=G.at[block(slot), cols],
            send_sem=sem,
            recv_sem=grecv.at[slot, h],
            device_id=target,
            device_id_type=MESH,
        )

    sibling = dev(a, b, 1 - c)

    def spread(h, s, d, upward, downward):
        slot = slot_of(a + d, b, c)
        if d:
            gcopy(slot, h, sibling, gc.at[s, 0, h]).wait_recv()
        if upward:

            @pl.when(a < A - 1)
            def _():
                gcopy(slot, h, dev(a + 1, b, c), gz.at[0, s, h]).start()

        if downward:

            @pl.when(a > 0)
            def _():
                gcopy(slot, h, dev(a - 1, b, c), gz.at[1, s, h]).start()

        for k in range(1, B):
            gcopy(slot, h, dev(a, around(b, k, B), c), gx.at[a + d, k, h]).start()
        gcopy(slot, h, sibling, gc.at[a + d, 0, h]).start()

    for s in range(A):
        for h in range(2):
            if s == 0:
                spread(h, 0, 0, True, True)
            else:

                @pl.when(a - s >= 0)
                def _():
                    spread(h, s, -s, True, False)

                @pl.when(a + s < A)
                def _():
                    spread(h, s, s, False, True)

    for s in range(A):
        for h in range(2):
            for sign in (-1, 1) if s else (1,):

                @pl.when((a + sign * s >= 0) & (a + sign * s < A))
                def _():
                    at = a + sign * s
                    for k in range(1, B):
                        copy = gcopy(slot_of(at, around(b, k, B), c), h, sibling, gc.at[at, k, h])
                        copy.wait_recv()
                        copy.start()

    for i in range(A):
        for k in range(B):
            for h in range(2):
                gcopy(slot_of(i, around(b, k, B), 1 - c), h, sibling, gc.at[i, k, h]).wait_recv()

    high = G[:, pl.ds(Dl, lanes)]
    low = G[:, pl.ds(Dl + lanes, lanes)]
    pick = (lax.broadcasted_iota(jnp.int32, (8, lanes), 1) == e).astype(F32).astype(BF)
    wrow = lax.dot_general(pick, high, nt, preferred_element_type=F32) + lax.dot_general(
        pick, low, nt, preferred_element_type=F32
    )
    sub = lax.broadcasted_iota(jnp.int32, (NT, NT), 0)
    lan = lax.broadcasted_iota(jnp.int32, (NT, NT), 1)
    same = (sub // tok) == (lan // tok)
    before_row = jnp.where(same & (sub < lan), 1.0, 0.0).astype(BF)
    before_col = jnp.where(same & (lan < sub), 1.0, 0.0).astype(BF)
    row_on = jnp.where(wrow > 0, 1.0, 0.0)
    row_pos = jnp.dot(row_on.astype(BF), before_row, preferred_element_type=F32)
    row_blk = (lax.broadcasted_iota(jnp.int32, (8, NT), 1) // tok * cap).astype(F32)
    row_at = jnp.where(wrow > 0, row_blk + row_pos, -1.0)[:1]
    slot_row = lax.broadcasted_iota(jnp.int32, (R, NT), 0).astype(F32)
    chosen = jnp.where(slot_row == row_at, 1.0, 0.0)
    wslot = jnp.sum(chosen * wrow[:1], axis=1, keepdims=True)
    S = chosen.astype(BF)

    mine = lax.broadcasted_iota(jnp.int32, (NT, lanes), 1) == e
    full = high.astype(F32) + low.astype(F32)
    all_on = jnp.where(full > 0, 1.0, 0.0)
    col_pos = jnp.dot(before_col, all_on.astype(BF), preferred_element_type=F32)
    col_blk = (lax.broadcasted_iota(jnp.int32, (NT, lanes), 0) // tok * cap).astype(F32)
    col_at = jnp.where(full > 0, col_blk + col_pos, -1.0)
    col_at = jnp.sum(jnp.where(mine, col_at, 0.0), axis=1, keepdims=True)
    slot_col = lax.broadcasted_iota(jnp.int32, (NT, R), 1).astype(F32)
    ST = jnp.where(slot_col == col_at, 1.0, 0.0).astype(BF)

    for copy in weight_copies:
        copy.wait()

    @pl.loop(0, nd)
    def _(j):
        cols = pl.ds(pl.multiple_of(j * dc, 128), dc)
        X[:, cols] = jnp.dot(S, G[:, cols], preferred_element_type=F32).astype(BF)

    def ycopy(p, j):
        return pltpu.make_async_remote_copy(
            src_ref=ysend.at[p - 1, j],
            dst_ref=yrecv.at[p - 1, j],
            send_sem=ys.at[p - 1, j],
            recv_sem=yr.at[p - 1, j],
            device_id=(e, around(t, p, T)),
            device_id_type=MESH,
        )

    def hcols(rank, j):
        return pl.ds(pl.multiple_of(rank * FT + j * fc, 128), fc)

    def hcopy(p, j, rank):
        return pltpu.make_async_remote_copy(
            src_ref=hid.at[:, hcols(rank, j)],
            dst_ref=hid.at[:, hcols(rank, j)],
            send_sem=hs.at[p - 1, j],
            recv_sem=hr.at[p - 1, j],
            device_id=(e, around(t, p, T)),
            device_id_type=MESH,
        )

    for p in range(1, T):

        @pl.loop(0, nj)
        def _(j):
            cols = hcols(around(t, p, T), j)
            g = jnp.dot(X[...], gw[:, cols], preferred_element_type=F32)
            u = jnp.dot(X[...], uw[:, cols], preferred_element_type=F32)
            ysend[p - 1, j, 0] = g.astype(BF)
            ysend[p - 1, j, 1] = u.astype(BF)
            ycopy(p, j).start()

    @pl.loop(0, nj)
    def _(j):
        cols = hcols(t, j)
        g = jnp.dot(X[...], gw[:, cols], preferred_element_type=F32)
        u = jnp.dot(X[...], uw[:, cols], preferred_element_type=F32)
        for p in range(1, T):
            ycopy(p, j).wait_recv()
            g += yrecv[p - 1, j, 0].astype(F32)
            u += yrecv[p - 1, j, 1].astype(F32)
        hid[:, cols] = (g / (1.0 + jnp.exp(-g)) * u).astype(BF)
        for p in range(1, T):
            hcopy(p, j, t).start()

    for p in range(1, T):
        for j in range(nj):
            hcopy(p, j, around(t, T - p, T)).wait_recv()

    def ccopy(j):
        return pltpu.make_async_remote_copy(
            src_ref=dense.at[j, 1 - c],
            dst_ref=crecv.at[j],
            send_sem=cs.at[j],
            recv_sem=cr.at[j],
            device_id=dev(a, b, 1 - c),
            device_id_type=MESH,
        )

    def xcopy(j, k):
        return pltpu.make_async_remote_copy(
            src_ref=s1.at[j, around(b, k, B)],
            dst_ref=xrecv.at[j, k - 1],
            send_sem=xs.at[j, k - 1],
            recv_sem=xr.at[j, k - 1],
            device_id=dev(a, around(b, k, B), c),
            device_id_type=MESH,
        )

    def zcopy(j, i):
        return pltpu.make_async_remote_copy(
            src_ref=s2.at[j, around(a, i, A)],
            dst_ref=zrecv.at[j, i - 1],
            send_sem=zs.at[j, i - 1],
            recv_sem=zr.at[j, i - 1],
            device_id=dev(around(a, i, A), b, c),
            device_id_type=MESH,
        )

    @pl.loop(0, nd + 4)
    def _(step):
        @pl.when(step < nd)
        def _():
            j = step
            rows = pl.ds(pl.multiple_of(j * dc, 128), dc)
            y = lax.dot_general(hid[...], dw[rows, :], nt, preferred_element_type=F32)
            y = (y * wslot).astype(BF)
            back = jnp.dot(ST, y, preferred_element_type=F32).astype(BF)
            for slot in range(E):
                at = (slot // 2 % B) * A + slot // (2 * B)
                dense[j, slot % 2, at * tok : (at + 1) * tok, :] = back[slot * tok : (slot + 1) * tok]
            ccopy(j).start()

        @pl.when((step >= 1) & (step < nd + 1))
        def _():
            j = step - 1
            ccopy(j).wait_recv()
            for k in range(B):
                at = pl.ds(k * A * tok, A * tok)
                s1[j, k] = (dense[j, c, at].astype(F32) + crecv[j, at].astype(F32)).astype(BF)
            for k in range(1, B):
                xcopy(j, k).start()

        @pl.when(step >= 4)
        def _():
            j = step - 4
            for k in range(1, B):
                xcopy(j, k).wait_recv()
            for i in range(A):
                at = pl.ds(i * tok, tok)
                total = s1[j, b, at].astype(F32)
                for k in range(1, B):
                    total += xrecv[j, k - 1, at].astype(F32)
                s2[j, i] = total.astype(BF)
            for i in range(1, A):
                zcopy(j, i).start()

    @pl.loop(0, nd)
    def _(j):
        total = s2[j, a].astype(F32)
        for i in range(1, A):
            zcopy(j, i).wait_recv()
            total += zrecv[j, i - 1].astype(F32)
        out_ref[:, pl.ds(pl.multiple_of(j * dc, 128), dc)] = total.astype(BF)

    for h in range(2):
        for s in range(A):

            @pl.when((a - s >= 0) & (a < A - 1))
            def _():
                gcopy(e, h, sibling, gz.at[0, s, h]).wait_send()

            @pl.when((a + s < A) & (a > 0))
            def _():
                gcopy(e, h, sibling, gz.at[1, s, h]).wait_send()

            for k in range(B):
                gcopy(e, h, sibling, gc.at[s, k, h]).wait_send()
                if k:
                    gcopy(e, h, sibling, gx.at[s, k, h]).wait_send()

    for p in range(1, T):
        for j in range(nj):
            ycopy(p, j).wait_send()
            hcopy(p, j, t).wait_send()

    @pl.loop(0, nd)
    def _(j):
        ccopy(j).wait_send()
        for k in range(1, B):
            xcopy(j, k).wait_send()
        for i in range(1, A):
            zcopy(j, i).wait_send()


def shards(tokens, routes, route_logits, gate_weight, up_weight, down_weight):
    E = lax.axis_size("expert")
    T = lax.axis_size("tensor")
    tok, D = tokens.shape
    top = routes.shape[1]
    _, Dl, F = gate_weight.shape
    cap = tok // 2
    A = 4
    B = E // (2 * A)
    assert E == A * B * 2 and D == Dl * T
    lanes = -(-E // 128) * 128
    nd = 7 if Dl % (7 * 128) == 0 else 1
    dc = Dl // nd
    FT = F // T
    fc = 128 if FT % 128 == 0 else FT
    nj = FT // fc
    pieces = 4
    R, NT = E * cap, E * tok
    dims = (E, T, A, B, tok, cap, top, Dl, F, lanes, nd, dc, fc, nj, pieces)
    vmem = pl.BlockSpec(memory_space=pltpu.VMEM)
    hbm = pl.BlockSpec(memory_space=pl.ANY)
    dma = pltpu.SemaphoreType.DMA
    return pl.pallas_call(
        functools.partial(kernel, dims),
        out_shape=jax.ShapeDtypeStruct((tok, Dl), BF),
        in_specs=[hbm, vmem, vmem, hbm, hbm, hbm],
        out_specs=vmem,
        scratch_shapes=[
            pltpu.VMEM((NT, Dl + 2 * lanes), BF),
            pltpu.VMEM((Dl, F), BF),
            pltpu.VMEM((Dl, F), BF),
            pltpu.VMEM((Dl, F), BF),
            pltpu.VMEM((R, Dl), BF),
            pltpu.VMEM((T - 1, nj, 2, R, fc), BF),
            pltpu.VMEM((T - 1, nj, 2, R, fc), BF),
            pltpu.VMEM((R, F), BF),
            pltpu.VMEM((nd, 2, A * B * tok, dc), BF),
            pltpu.VMEM((nd, A * B * tok, dc), BF),
            pltpu.VMEM((nd, B, A * tok, dc), BF),
            pltpu.VMEM((nd, B - 1, A * tok, dc), BF),
            pltpu.VMEM((nd, A, tok, dc), BF),
            pltpu.VMEM((nd, A - 1, tok, dc), BF),
            dma((3, pieces)),
            dma((2,)),
            dma((E, 2)),
            dma((2, A, 2)),
            dma((A, B, 2)),
            dma((A, B, 2)),
            dma((T - 1, nj)),
            dma((T - 1, nj)),
            dma((T - 1, nj)),
            dma((T - 1, nj)),
            dma((nd,)),
            dma((nd,)),
            dma((nd, B - 1)),
            dma((nd, B - 1)),
            dma((nd, A - 1)),
            dma((nd, A - 1)),
        ],
        compiler_params=pltpu.CompilerParams(
            collective_id=0, has_side_effects=True, vmem_limit_bytes=60 * 1024 * 1024
        ),
    )(tokens, routes.T, route_logits.T, gate_weight, up_weight, down_weight)


def solution(mesh):
    return jax.shard_map(
        shards,
        mesh=mesh,
        in_specs=(
            P("expert", None),
            P("expert", None),
            P("expert", None),
            P("expert", "tensor", None),
            P("expert", "tensor", None),
            P("expert", "tensor", None),
        ),
        out_specs=P("expert", "tensor"),
        check_vma=False,
    )
```

```python
import functools

import jax
import jax.numpy as jnp
from jax import lax
from jax.experimental import pallas as pl
from jax.experimental.pallas import tpu as pltpu
from jax.sharding import PartitionSpec as P

routed_scale = 2.5
MESH = pl.DeviceIdType.MESH
BF = jnp.bfloat16
F32 = jnp.float32
NT_DIMS = (((1,), (1,)), ((), ()))
CORE_LAG, X_LAG, Z_LAG = 2, 6, 9
HELD = 0


def kernel(
    dims,
    tokens_ref,
    routes_hbm,
    logits_hbm,
    gate_hbm,
    up_hbm,
    down_hbm,
    out_ref,
    routes_ref,
    logits_ref,
    G,
    gw,
    uw,
    dw,
    X,
    spread_back,
    wslot,
    ysend,
    yrecv,
    acc,
    hid,
    dense,
    crecv,
    s1,
    xrecv,
    s2,
    z1recv,
    s3,
    z2recv,
    rsem,
    wsem,
    tsem,
    gs,
    gzr,
    gxr,
    gcr,
    ys,
    yr,
    hs,
    hr,
    cs,
    cr,
    xs,
    xr,
    z1s,
    z1r,
    z2s,
    z2r,
):
    E, T, A, B, tok, cap, top, Dl, F, lanes, hc, nd, dc, fc, nj, pieces = dims
    slots = 2 * B * 2
    NG, RG, FT = slots * tok, slots * cap, F // T
    hw = Dl // hc
    e = lax.axis_index("expert")
    t = lax.axis_index("tensor")
    c = lax.rem(e, 2)
    b = lax.rem(e // 2, B)
    a = e // (2 * B)
    r = lax.rem(a, 2)
    half = a // 2
    near = a + 1 - 2 * r
    far = a + 2 - 4 * half
    places = (a, near, far, far + 1 - 2 * r)

    def around(v, i, n):
        return lax.rem(v + i, n)

    def slot_of(ai, bi, ci):
        return (ai * B + bi) * 2 + ci

    def dev(ai, bi, ci):
        return (slot_of(ai, bi, ci), t)

    sibling = dev(a, b, 1 - c)
    z1, z2 = dev(near, b, c), dev(far, b, c)

    barrier = pltpu.get_barrier_semaphore()
    partners = [z1, z2, sibling]
    partners += [dev(a, around(b, k, B), c) for k in range(1, B)]
    partners += [(e, around(t, p, T)) for p in range(1, T)]
    for partner in partners:
        pl.semaphore_signal(barrier, inc=1, device_id=partner, device_id_type=MESH)

    def block(slot):
        return pl.ds(pl.multiple_of(slot * tok, tok), tok)

    route_copies = []
    for which, (src, dst) in enumerate(((routes_hbm, routes_ref), (logits_hbm, logits_ref))):
        copy = pltpu.make_async_copy(src, dst, rsem.at[which])
        copy.start()
        route_copies.append(copy)
    token_copies = []
    for h in range(hc):
        copy = pltpu.make_async_copy(
            tokens_ref.at[:, pl.ds(pl.multiple_of(t * Dl + h * hw, 128), hw)],
            G.at[block(e), pl.ds(lanes + h * hw, hw)],
            tsem.at[h],
        )
        copy.start()
        token_copies.append(copy)

    low_at = lanes // 2
    for copy in route_copies:
        copy.wait()
    scores = jax.nn.sigmoid(logits_ref[...])
    weights = routed_scale * scores / jnp.sum(scores, axis=0, keepdims=True)
    routes = routes_ref[...]
    lane = lax.broadcasted_iota(jnp.int32, (low_at, tok), 0)
    table = jnp.zeros((low_at, tok), F32)
    for k in range(top):
        table += jnp.where(lane == routes[k : k + 1], weights[k : k + 1], 0.0)
    high = table.astype(BF)
    low = (table - high.astype(F32)).astype(BF)
    unit = lax.broadcasted_iota(jnp.int32, (tok, tok), 0) == lax.broadcasted_iota(jnp.int32, (tok, tok), 1)
    unit = jnp.where(unit, 1.0, 0.0).astype(BF)
    both = jnp.concatenate([high, low], axis=0)
    G[block(e), pl.ds(0, lanes)] = lax.dot_general(unit, both, NT_DIMS, preferred_element_type=F32).astype(BF)

    sub = lax.broadcasted_iota(jnp.int32, (NG, NG), 0)
    lan = lax.broadcasted_iota(jnp.int32, (NG, NG), 1)
    same = (sub // tok) == (lan // tok)
    before_row = jnp.where(same & (sub < lan), 1.0, 0.0).astype(BF)
    before_col = jnp.where(same & (lan < sub), 1.0, 0.0).astype(BF)

    pl.semaphore_wait(barrier, len(partners))

    def part(h):
        if isinstance(h, int) and h == 0:
            return pl.ds(0, lanes + hw)
        return pl.ds(pl.multiple_of(lanes + h * hw, 128), hw)

    def gcopy(slot, h, target, sem):
        return pltpu.make_async_remote_copy(
            src_ref=G.at[block(slot), part(h)],
            dst_ref=G.at[block(slot), part(h)],
            send_sem=gs,
            recv_sem=sem,
            device_id=target,
            device_id_type=MESH,
        )

    def gwait(h, sem, count=1):
        span = G.at[pl.ds(0, count * tok), part(h)]
        pltpu.make_async_copy(span, span, sem).wait()

    def across(i, h):
        slot = slot_of(places[i], b, c)
        for k in range(1, B):
            gcopy(slot, h, dev(a, around(b, k, B), c), gxr.at[i, k - 1, h]).start()
        gcopy(slot, h, sibling, gcr.at[i // 2, h]).start()

    def relay(i, h):
        for k in range(1, B):
            gwait(h, gxr.at[i, k - 1, h])
            gcopy(slot_of(places[i], around(b, B - k, B), c), h, sibling, gcr.at[i // 2, h]).start()

    for h in range(hc):
        token_copies[h].wait()
        gcopy(e, h, z1, gzr.at[0, h]).start()
        across(0, h)

    step_in = Dl // pieces
    for which, (src, dst) in enumerate(((gate_hbm, gw), (up_hbm, uw), (down_hbm, dw))):
        for p in range(pieces):
            rows = pl.ds(p * step_in, step_in)
            pltpu.make_async_copy(src.at[0, rows], dst.at[rows], wsem.at[which]).start()

    def weight_ready(which, src, dst):
        pltpu.make_async_copy(src.at[0], dst, wsem.at[which]).wait()

    for h in range(hc):
        gwait(h, gzr.at[0, h])
        across(1, h)
        gcopy(e, h, z2, gzr.at[1, h]).start()
        relay(0, h)

    for h in range(hc):
        gwait(h, gzr.at[1, h])
        gcopy(slot_of(far, b, c), h, z1, gzr.at[2, h]).start()
        across(2, h)
        relay(1, h)

    def relay_far(h):
        gwait(h, gzr.at[2, h])
        across(3, h)
        relay(2, h)

    def relay_last(h):
        relay(3, h)

    def group_rows(g):
        return pl.ds(pl.multiple_of((half if g == 0 else 1 - half) * NG, NG), NG)

    def choose(g):
        meta = G[group_rows(g), pl.ds(0, lanes)]
        at = lax.broadcasted_iota(jnp.int32, (8, lanes), 1)
        pick = jnp.where((at == e) | (at == e + low_at), 1.0, 0.0).astype(BF)
        wrow = lax.dot_general(pick, meta, NT_DIMS, preferred_element_type=F32)
        row_on = jnp.where(wrow > 0, 1.0, 0.0)
        row_pos = jnp.dot(row_on.astype(BF), before_row, preferred_element_type=F32)
        row_blk = (lax.broadcasted_iota(jnp.int32, (8, NG), 1) // tok * cap).astype(F32)
        row_at = jnp.where(wrow > 0, row_blk + row_pos, -1.0)[:1]
        slot_row = lax.broadcasted_iota(jnp.int32, (RG, NG), 0).astype(F32)
        S = jnp.where(slot_row == row_at, 1.0, 0.0).astype(BF)

        full = meta.astype(F32)
        at = lax.broadcasted_iota(jnp.int32, (NG, lanes), 1)
        all_on = jnp.where(full > 0, 1.0, 0.0)
        col_pos = jnp.dot(before_col, all_on.astype(BF), preferred_element_type=F32)
        col_blk = (lax.broadcasted_iota(jnp.int32, (NG, lanes), 0) // tok * cap).astype(F32)
        col_at = jnp.where(full > 0, col_blk + col_pos, -1.0)
        col_at = jnp.sum(jnp.where(at == e, col_at, 0.0), axis=1, keepdims=True)
        slot_col = lax.broadcasted_iota(jnp.int32, (NG, RG), 1).astype(F32)
        spread_back[g] = jnp.where(slot_col == col_at, 1.0, 0.0).astype(BF)
        mine = (at == e) | (at == e + low_at)
        wcol = jnp.sum(jnp.where(mine, full, 0.0), axis=1, keepdims=True)
        wslot[g] = jnp.sum(jnp.where(slot_col == col_at, wcol, 0.0), axis=0, keepdims=True)
        return S

    chosen = [None, None]

    def collect(g, h):
        gwait(h, gcr.at[g, h], 2 * B)
        if h == 0:
            chosen[g] = choose(g)
        rows = G[group_rows(g), pl.ds(lanes + h * hw, hw)]
        X[g, :, pl.ds(h * hw, hw)] = jnp.dot(chosen[g], rows, preferred_element_type=F32).astype(BF)

    def ycopy(g, p, j):
        return pltpu.make_async_remote_copy(
            src_ref=ysend.at[g, p - 1, j],
            dst_ref=yrecv.at[g, p - 1, j],
            send_sem=ys,
            recv_sem=yr.at[g, p - 1, j],
            device_id=(e, around(t, p, T)),
            device_id_type=MESH,
        )

    def hcols(rank, j):
        return pl.ds(pl.multiple_of(rank * FT + j * fc, 128), fc)

    def hcopy(g, p, j, rank):
        return pltpu.make_async_remote_copy(
            src_ref=hid.at[g, :, hcols(rank, j)],
            dst_ref=hid.at[g, :, hcols(rank, j)],
            send_sem=hs,
            recv_sem=hr.at[g],
            device_id=(e, around(t, p, T)),
            device_id_type=MESH,
        )

    def gate_up_theirs(g, j):
        for p in range(1, T):
            cols = hcols(around(t, p, T), j)
            ysend[g, p - 1, j, 0] = jnp.dot(X[g], gw[:, cols], preferred_element_type=F32).astype(BF)
            ysend[g, p - 1, j, 1] = jnp.dot(X[g], uw[:, cols], preferred_element_type=F32).astype(BF)
            ycopy(g, p, j).start()

    def gate_up_own(g, j):
        cols = hcols(t, j)
        acc[g, j, 0] = jnp.dot(X[g], gw[:, cols], preferred_element_type=F32)
        acc[g, j, 1] = jnp.dot(X[g], uw[:, cols], preferred_element_type=F32)

    def hidden(g, j):
        gv, uv = acc[g, j, 0], acc[g, j, 1]
        for p in range(1, T):
            ycopy(g, p, j).wait_recv()
            gv += yrecv[g, p - 1, j, 0].astype(F32)
            uv += yrecv[g, p - 1, j, 1].astype(F32)
        hid[g, :, hcols(t, j)] = (gv / (1.0 + jnp.exp(-gv)) * uv).astype(BF)
        for p in range(1, T):
            hcopy(g, p, j, t).start()

    def hidden_ready(g):
        span = hid.at[g, :, pl.ds(0, F - FT)]
        pltpu.make_async_copy(span, span, hr.at[g]).wait()

    def spread_over(work, side):
        for i, item in enumerate(work):
            item()
            for other in side[i * len(side) // len(work) : (i + 1) * len(side) // len(work)]:
                other()

    def each(fn, n, *lead):
        return [functools.partial(fn, *lead, i) for i in range(n)]

    for h in range(hc):
        collect(0, h)
    weight_ready(0, gate_hbm, gw)
    weight_ready(1, up_hbm, uw)
    spread_over(each(gate_up_theirs, nj, 0), each(relay_far, hc))
    for j in range(nj):
        gate_up_own(0, j)
    spread_over(each(relay_last, hc), each(hidden, nj, 0))
    for h in range(hc):
        collect(1, h)
    for j in range(nj):
        gate_up_theirs(1, j)

    def ccopy(j):
        return pltpu.make_async_remote_copy(
            src_ref=dense.at[j, 1 - c],
            dst_ref=crecv.at[j],
            send_sem=cs,
            recv_sem=cr.at[j],
            device_id=sibling,
            device_id_type=MESH,
        )

    def xcopy(j, k):
        return pltpu.make_async_remote_copy(
            src_ref=s1.at[j, around(b, k, B)],
            dst_ref=xrecv.at[j, k - 1],
            send_sem=xs,
            recv_sem=xr.at[j],
            device_id=dev(a, around(b, k, B), c),
            device_id_type=MESH,
        )

    def z1copy(j):
        return pltpu.make_async_remote_copy(
            src_ref=s2.at[j, 1 - r],
            dst_ref=z1recv.at[j],
            send_sem=z1s,
            recv_sem=z1r.at[j],
            device_id=z1,
            device_id_type=MESH,
        )

    def z2copy(j):
        return pltpu.make_async_remote_copy(
            src_ref=s3.at[j],
            dst_ref=z2recv.at[j],
            send_sem=z2s,
            recv_sem=z2r.at[j],
            device_id=z2,
            device_id_type=MESH,
        )

    total_steps = 2 * nd
    nd_before = max(nd - HELD, 1)

    def down(g, step, early=True):
        j = step - nd_before if g else step if early else step - nd
        rows = pl.ds(pl.multiple_of(j * dc, 128), dc)
        y = lax.dot_general(dw[rows, :], hid[g], NT_DIMS, preferred_element_type=F32)
        y = (y * wslot[g]).astype(BF)
        y = lax.dot_general(spread_back[g], y, NT_DIMS, preferred_element_type=F32).astype(BF)
        for slot in range(slots):
            at = (slot // 2 % B) * 2 + slot // (2 * B)
            dense[step, slot % 2, at * tok : (at + 1) * tok, :] = y[slot * tok : (slot + 1) * tok]
        ccopy(step).start()

    def reduce_steps(step):
        @pl.when((step >= CORE_LAG) & (step < total_steps + CORE_LAG))
        def _():
            j = step - CORE_LAG
            ccopy(j).wait_recv()
            for k in range(B):
                at = pl.ds(k * 2 * tok, 2 * tok)
                s1[j, k] = (dense[j, c, at].astype(F32) + crecv[j, at].astype(F32)).astype(BF)
            for k in range(1, B):
                xcopy(j, k).start()

        @pl.when((step >= X_LAG) & (step < total_steps + X_LAG))
        def _():
            j = step - X_LAG
            pltpu.make_async_copy(xrecv.at[j], xrecv.at[j], xr.at[j]).wait()
            for i in range(2):
                at = pl.ds(i * tok, tok)
                total = s1[j, b, at].astype(F32)
                for k in range(1, B):
                    total += xrecv[j, k - 1, at].astype(F32)
                s2[j, i] = total.astype(BF)
            z1copy(j).start()

        @pl.when((step >= Z_LAG + nd_before) & (step < nd_before + nd + Z_LAG))
        def _():
            j = step - Z_LAG
            z1copy(j).wait_recv()
            s3[j - nd_before] = (s2[j, r].astype(F32) + z1recv[j].astype(F32)).astype(BF)
            z2copy(j - nd_before).start()

    hidden_ready(0)
    weight_ready(2, down_hbm, dw)

    extra = each(gate_up_own, nj, 1) + each(hidden, nj, 1)

    @pl.loop(0, nd_before)
    def _(step):
        down(0, step)
        reduce_steps(step)
        for i, item in enumerate(extra):
            pl.when(step == min(i + 1, nd_before - 1))(item)

    hidden_ready(1)

    @pl.loop(nd_before, nd_before + nd)
    def _(step):
        down(1, step)
        reduce_steps(step)

    if nd_before < nd:

        @pl.loop(nd_before + nd, total_steps)
        def _(step):
            down(0, step, False)
            reduce_steps(step)

    @pl.loop(total_steps, total_steps + Z_LAG)
    def _(step):
        reduce_steps(step)

    for j in range(nd):
        near_at = j if j < nd_before else j + nd
        z1copy(near_at).wait_recv()
        z2copy(j).wait_recv()
        total = s2[near_at, r].astype(F32) + z1recv[near_at].astype(F32) + z2recv[j].astype(F32)
        out_ref[:, pl.ds(j * dc, dc)] = total.astype(BF)

    def sent(ref, sem):
        pltpu.make_async_copy(ref, ref, sem).wait()

    sent(G.at[pl.ds(0, (3 + A * (2 * B - 1)) * tok)], gs)
    sent(ysend, ys)
    sent(hid.at[:, :, pl.ds(0, F - FT)], hs)
    sent(crecv, cs)
    sent(xrecv, xs)
    sent(z1recv, z1s)
    sent(z2recv, z2s)


def shards(tokens, routes, route_logits, gate_weight, up_weight, down_weight):
    E = lax.axis_size("expert")
    T = lax.axis_size("tensor")
    tok, D = tokens.shape
    top = routes.shape[1]
    _, Dl, F = gate_weight.shape
    cap = tok // 2
    A = 4
    B = E // (2 * A)
    assert E == A * B * 2 and D == Dl * T
    lanes = -(-2 * E // 128) * 128
    hc = 4 if Dl % (4 * 128) == 0 else 1
    nd = 7 if Dl % (7 * 128) == 0 else 1
    dc = Dl // nd
    FT = F // T
    fc = 256 if FT % 256 == 0 else FT
    nj = FT // fc
    pieces = 4
    NG, RG = 4 * B * tok, 4 * B * cap
    dims = (E, T, A, B, tok, cap, top, Dl, F, lanes, hc, nd, dc, fc, nj, pieces)
    vmem = pl.BlockSpec(memory_space=pltpu.VMEM)
    hbm = pl.BlockSpec(memory_space=pl.ANY)
    dma = pltpu.SemaphoreType.DMA
    return pl.pallas_call(
        functools.partial(kernel, dims),
        out_shape=pltpu.VMEM((tok, Dl), BF),
        in_specs=[hbm] * 6,
        out_specs=vmem,
        scratch_shapes=[
            pltpu.VMEM((top, tok), jnp.int32),
            pltpu.VMEM((top, tok), F32),
            pltpu.VMEM((2 * NG, lanes + Dl), BF),
            pltpu.VMEM((Dl, F), BF),
            pltpu.VMEM((Dl, F), BF),
            pltpu.VMEM((Dl, F), BF),
            pltpu.VMEM((2, RG, Dl), BF),
            pltpu.VMEM((2, NG, RG), BF),
            pltpu.VMEM((2, 1, RG), F32),
            pltpu.VMEM((2, T - 1, nj, 2, RG, fc), BF),
            pltpu.VMEM((2, T - 1, nj, 2, RG, fc), BF),
            pltpu.VMEM((2, nj, 2, RG, fc), F32),
            pltpu.VMEM((2, RG, F), BF),
            pltpu.VMEM((2 * nd, 2, NG // 2, dc), BF),
            pltpu.VMEM((2 * nd, NG // 2, dc), BF),
            pltpu.VMEM((2 * nd, B, 2 * tok, dc), BF),
            pltpu.VMEM((2 * nd, B - 1, 2 * tok, dc), BF),
            pltpu.VMEM((2 * nd, 2, tok, dc), BF),
            pltpu.VMEM((2 * nd, tok, dc), BF),
            pltpu.VMEM((nd, tok, dc), BF),
            pltpu.VMEM((nd, tok, dc), BF),
            dma((2,)),
            dma((3,)),
            dma((hc,)),
            dma,
            dma((3, hc)),
            dma((A, B - 1, hc)),
            dma((2, hc)),
            dma,
            dma((2, T - 1, nj)),
            dma,
            dma((2,)),
            dma,
            dma((2 * nd,)),
            dma,
            dma((2 * nd,)),
            dma,
            dma((2 * nd,)),
            dma,
            dma((nd,)),
        ],
        compiler_params=pltpu.CompilerParams(
            collective_id=0, has_side_effects=True, vmem_limit_bytes=60 * 1024 * 1024
        ),
    )(tokens, routes.T, route_logits.T, gate_weight, up_weight, down_weight)


def solution(mesh):
    return jax.shard_map(
        shards,
        mesh=mesh,
        in_specs=(
            P("expert", None),
            P("expert", None),
            P("expert", None),
            P("expert", "tensor", None),
            P("expert", "tensor", None),
            P("expert", "tensor", None),
        ),
        out_specs=P("expert", "tensor"),
        check_vma=False,
    )
```

```python
import functools

import jax
import jax.numpy as jnp
from jax import lax
from jax.experimental import pallas as pl
from jax.experimental.pallas import tpu as pltpu
from jax.sharding import PartitionSpec as P

routed_scale = 2.5
MESH = pl.DeviceIdType.MESH
BF = jnp.bfloat16
F32 = jnp.float32
NT_DIMS = (((1,), (1,)), ((), ()))
CORE_LAG, X_LAG, Z_LAG = 2, 6, 9
HELD = 0


def kernel(
    dims,
    tokens_ref,
    routes_hbm,
    logits_hbm,
    gate_hbm,
    up_hbm,
    down_hbm,
    out_ref,
    routes_ref,
    logits_ref,
    G,
    gw,
    uw,
    dw,
    X,
    spread_back,
    wcol,
    ysend,
    yrecv,
    acc,
    kept_part,
    hid,
    hid_rows,
    dense,
    crecv,
    s1,
    xrecv,
    s2,
    z1recv,
    s3,
    z2recv,
    rsem,
    wsem,
    tsem,
    gs,
    gzr,
    gxr,
    gvr,
    gcr,
    ys,
    yr,
    hs,
    hr,
    cs,
    cr,
    xs,
    xr,
    z1s,
    z1r,
    z2s,
    z2r,
):
    E, T, A, B, tok, cap, top, Dl, F, lanes, hc, nd, dc, fc, nj, pieces = dims
    slots = 2 * B * 2
    NG, RG, FT = slots * tok, slots * cap, F // T
    hw = Dl // hc
    e = lax.axis_index("expert")
    t = lax.axis_index("tensor")
    c = lax.rem(e, 2)
    b = lax.rem(e // 2, B)
    a = e // (2 * B)
    r = lax.rem(a, 2)
    half = a // 2
    near = a + 1 - 2 * r
    far = a + 2 - 4 * half
    places = (a, near, far, far + 1 - 2 * r)

    def around(v, i, n):
        return lax.rem(v + i, n)

    def slot_of(ai, bi, ci):
        return (ai * B + bi) * 2 + ci

    def dev(ai, bi, ci):
        return (slot_of(ai, bi, ci), t)

    sibling = dev(a, b, 1 - c)
    z1, z2 = dev(near, b, c), dev(far, b, c)

    barrier = pltpu.get_barrier_semaphore()
    partners = [z1, z2, sibling]
    partners += [dev(a, around(b, k, B), c) for k in range(1, B)]
    partners += [(e, around(t, p, T)) for p in range(1, T)]
    for partner in partners:
        pl.semaphore_signal(barrier, inc=1, device_id=partner, device_id_type=MESH)

    def block(slot):
        return pl.ds(pl.multiple_of(slot * tok, tok), tok)

    route_copies = []
    for which, (src, dst) in enumerate(((routes_hbm, routes_ref), (logits_hbm, logits_ref))):
        copy = pltpu.make_async_copy(src, dst, rsem.at[which])
        copy.start()
        route_copies.append(copy)
    token_copies = []
    for h in range(hc):
        copy = pltpu.make_async_copy(
            tokens_ref.at[:, pl.ds(pl.multiple_of(t * Dl + h * hw, 128), hw)],
            G.at[block(e), pl.ds(lanes + h * hw, hw)],
            tsem.at[h],
        )
        copy.start()
        token_copies.append(copy)

    low_at = lanes // 2
    for copy in route_copies:
        copy.wait()
    scores = jax.nn.sigmoid(logits_ref[...])
    weights = routed_scale * scores / jnp.sum(scores, axis=0, keepdims=True)
    routes = routes_ref[...]
    lane = lax.broadcasted_iota(jnp.int32, (low_at, tok), 0)
    table = jnp.zeros((low_at, tok), F32)
    for k in range(top):
        table += jnp.where(lane == routes[k : k + 1], weights[k : k + 1], 0.0)
    high = table.astype(BF)
    low = (table - high.astype(F32)).astype(BF)
    unit = lax.broadcasted_iota(jnp.int32, (tok, tok), 0) == lax.broadcasted_iota(jnp.int32, (tok, tok), 1)
    unit = jnp.where(unit, 1.0, 0.0).astype(BF)
    both = jnp.concatenate([high, low], axis=0)
    G[block(e), pl.ds(0, lanes)] = lax.dot_general(unit, both, NT_DIMS, preferred_element_type=F32).astype(BF)

    sub = lax.broadcasted_iota(jnp.int32, (NG, NG), 0)
    lan = lax.broadcasted_iota(jnp.int32, (NG, NG), 1)
    same = (sub // tok) == (lan // tok)
    before_row = jnp.where(same & (sub < lan), 1.0, 0.0).astype(BF)
    before_col = jnp.where(same & (lan < sub), 1.0, 0.0).astype(BF)

    pl.semaphore_wait(barrier, len(partners))

    def part(h):
        if isinstance(h, int) and h == 0:
            return pl.ds(0, lanes + hw)
        return pl.ds(pl.multiple_of(lanes + h * hw, 128), hw)

    def gcopy(slot, h, target, sem):
        return pltpu.make_async_remote_copy(
            src_ref=G.at[block(slot), part(h)],
            dst_ref=G.at[block(slot), part(h)],
            send_sem=gs,
            recv_sem=sem,
            device_id=target,
            device_id_type=MESH,
        )

    def gwait(h, sem, count=1):
        span = G.at[pl.ds(0, count * tok), part(h)]
        pltpu.make_async_copy(span, span, sem).wait()

    def by_z(h):
        return h % 2 == 1

    def across(i, h):
        slot = slot_of(places[i], b, c)
        for k in range(1, B) if i < 3 or not by_z(h) else ():
            gcopy(slot, h, dev(a, around(b, k, B), c), gxr.at[i, k - 1, h]).start()
        gcopy(slot, h, sibling, gcr.at[i // 2, h]).start()

    def relay(i, h):
        for k in range(1, B):
            sem = gvr.at[k - 1, h] if i == 3 and by_z(h) else gxr.at[i, k - 1, h]
            slot = slot_of(places[i], around(b, B - k, B), c)
            gwait(h, sem)
            if i == 2 and by_z(h):
                gcopy(slot, h, z1, gvr.at[k - 1, h]).start()
            gcopy(slot, h, sibling, gcr.at[i // 2, h]).start()

    for h in range(hc):
        token_copies[h].wait()
        gcopy(e, h, z1, gzr.at[0, h]).start()
        across(0, h)

    def own_far(h):
        gcopy(e, h, z2, gzr.at[1, h]).start()

    @pl.when(r == half)
    def _():
        for h in range(hc):
            own_far(h)


    step_in = Dl // pieces
    for which, (src, dst) in enumerate(((gate_hbm, gw), (up_hbm, uw), (down_hbm, dw))):
        for p in range(pieces):
            rows = pl.ds(p * step_in, step_in)
            pltpu.make_async_copy(src.at[0, rows], dst.at[rows], wsem.at[which]).start()

    def weight_ready(which, src, dst):
        pltpu.make_async_copy(src.at[0], dst, wsem.at[which]).wait()

    for h in range(hc):
        gwait(h, gzr.at[0, h])
        across(1, h)
        pl.when(r != half)(functools.partial(own_far, h))
        relay(0, h)

    for h in range(hc):
        gwait(h, gzr.at[1, h])
        gcopy(slot_of(far, b, c), h, z1, gzr.at[2, h]).start()
        across(2, h)
        relay(1, h)

    def relay_far(h):
        gwait(h, gzr.at[2, h])
        across(3, h)
        relay(2, h)

    def relay_last(h):
        relay(3, h)

    def group_rows(g):
        return pl.ds(pl.multiple_of((half if g == 0 else 1 - half) * NG, NG), NG)

    def choose(g):
        meta = G[group_rows(g), pl.ds(0, lanes)]
        at = lax.broadcasted_iota(jnp.int32, (8, lanes), 1)
        pick = jnp.where((at == e) | (at == e + low_at), 1.0, 0.0).astype(BF)
        wrow = lax.dot_general(pick, meta, NT_DIMS, preferred_element_type=F32)
        row_on = jnp.where(wrow > 0, 1.0, 0.0)
        row_pos = jnp.dot(row_on.astype(BF), before_row, preferred_element_type=F32)
        row_blk = (lax.broadcasted_iota(jnp.int32, (8, NG), 1) // tok * cap).astype(F32)
        row_at = jnp.where(wrow > 0, row_blk + row_pos, -1.0)[:1]
        slot_row = lax.broadcasted_iota(jnp.int32, (RG, NG), 0).astype(F32)
        S = jnp.where(slot_row == row_at, 1.0, 0.0).astype(BF)

        full = meta.astype(F32)
        at = lax.broadcasted_iota(jnp.int32, (NG, lanes), 1)
        all_on = jnp.where(full > 0, 1.0, 0.0)
        col_pos = jnp.dot(before_col, all_on.astype(BF), preferred_element_type=F32)
        col_blk = (lax.broadcasted_iota(jnp.int32, (NG, lanes), 0) // tok * cap).astype(F32)
        col_at = jnp.where(full > 0, col_blk + col_pos, -1.0)
        col_at = jnp.sum(jnp.where(at == e, col_at, 0.0), axis=1, keepdims=True)
        slot_col = lax.broadcasted_iota(jnp.int32, (NG, RG), 1).astype(F32)
        spread_back[g] = jnp.where(slot_col == col_at, 1.0, 0.0).astype(BF)
        mine = (at == e) | (at == e + low_at)
        wcol[g] = jnp.sum(jnp.where(mine, full, 0.0), axis=1, keepdims=True)
        return S

    chosen = [None, None]

    def collect(g, h):
        gwait(h, gcr.at[g, h], 2 * B)
        if h == 0:
            chosen[g] = choose(g)
        rows = G[group_rows(g), pl.ds(lanes + h * hw, hw)]
        X[g, :, pl.ds(h * hw, hw)] = jnp.dot(chosen[g], rows, preferred_element_type=F32).astype(BF)

    def ycopy(g, p, j):
        return pltpu.make_async_remote_copy(
            src_ref=ysend.at[g, p - 1, j],
            dst_ref=yrecv.at[g, p - 1, j],
            send_sem=ys,
            recv_sem=yr.at[g, p - 1, j],
            device_id=(e, around(t, p, T)),
            device_id_type=MESH,
        )

    def hcols(rank, j):
        return pl.ds(pl.multiple_of(rank * FT + j * fc, 128), fc)

    def hcopy(g, p, j, rank):
        return pltpu.make_async_remote_copy(
            src_ref=hid.at[g, :, hcols(rank, j)],
            dst_ref=hid.at[g, :, hcols(rank, j)],
            send_sem=hs,
            recv_sem=hr.at[g],
            device_id=(e, around(t, p, T)),
            device_id_type=MESH,
        )

    def gate_up_theirs(g, j, first=0, kept=False):
        depth = pl.ds(first, Dl - first)
        for p in range(1, T):
            cols = hcols(around(t, p, T), j)
            for which, w in enumerate((gw, uw)):
                value = jnp.dot(X[g, :, depth], w[depth, cols], preferred_element_type=F32)
                if kept:
                    value += kept_part[p - 1, j, which]
                ysend[g, p - 1, j, which] = value.astype(BF)
            ycopy(g, p, j).start()

    def gate_up_part(g, j, until):
        depth = pl.ds(0, until)
        for p in range(1, T):
            cols = hcols(around(t, p, T), j)
            for which, w in enumerate((gw, uw)):
                kept_part[p - 1, j, which] = jnp.dot(X[g, :, depth], w[depth, cols], preferred_element_type=F32)

    def gate_up_own(g, j):
        cols = hcols(t, j)
        acc[g, j, 0] = jnp.dot(X[g], gw[:, cols], preferred_element_type=F32)
        acc[g, j, 1] = jnp.dot(X[g], uw[:, cols], preferred_element_type=F32)

    def hidden(g, j):
        gv, uv = acc[g, j, 0], acc[g, j, 1]
        for p in range(1, T):
            ycopy(g, p, j).wait_recv()
            gv += yrecv[g, p - 1, j, 0].astype(F32)
            uv += yrecv[g, p - 1, j, 1].astype(F32)
        hid[g, :, hcols(t, j)] = (gv / (1.0 + jnp.exp(-gv)) * uv).astype(BF)
        for p in range(1, T):
            hcopy(g, p, j, t).start()

    def hidden_ready(g):
        span = hid.at[g, :, pl.ds(0, F - FT)]
        pltpu.make_async_copy(span, span, hr.at[g]).wait()
        hid_rows[g] = jnp.dot(spread_back[g], hid[g], preferred_element_type=F32).astype(BF)

    for h in range(hc):
        collect(0, h)
    weight_ready(0, gate_hbm, gw)
    weight_ready(1, up_hbm, uw)
    def run(*items):
        for item in items:
            item()

    def each(fn, n, *lead):
        return [functools.partial(fn, *lead, i) for i in range(n)]

    last, finish = each(relay_last, hc), each(hidden, nj, 0)
    cut = hc // 2
    run(*each(gate_up_theirs, nj, 0))
    run(*each(relay_far, hc))
    run(*each(gate_up_own, nj, 0))
    run(*last[:cut])
    run(*finish[:1])
    run(*last[cut:])
    for h in range(cut):
        collect(1, h)
    run(*finish[1:])
    for j in range(nj if cut else 0):
        gate_up_part(1, j, cut * hw)
    for h in range(cut, hc):
        collect(1, h)
    for j in range(nj):
        gate_up_theirs(1, j, cut * hw, bool(cut))
    run(*each(gate_up_own, nj, 1))

    def ccopy(j):
        return pltpu.make_async_remote_copy(
            src_ref=dense.at[j, 1 - c],
            dst_ref=crecv.at[j],
            send_sem=cs,
            recv_sem=cr.at[j],
            device_id=sibling,
            device_id_type=MESH,
        )

    def xcopy(j, k):
        return pltpu.make_async_remote_copy(
            src_ref=s1.at[j, around(b, k, B)],
            dst_ref=xrecv.at[j, k - 1],
            send_sem=xs,
            recv_sem=xr.at[j],
            device_id=dev(a, around(b, k, B), c),
            device_id_type=MESH,
        )

    def z1copy(j):
        return pltpu.make_async_remote_copy(
            src_ref=s2.at[j, 1 - r],
            dst_ref=z1recv.at[j],
            send_sem=z1s,
            recv_sem=z1r.at[j],
            device_id=z1,
            device_id_type=MESH,
        )

    def z2copy(j):
        return pltpu.make_async_remote_copy(
            src_ref=s3.at[j],
            dst_ref=z2recv.at[j],
            send_sem=z2s,
            recv_sem=z2r.at[j],
            device_id=z2,
            device_id_type=MESH,
        )

    total_steps = 2 * nd
    nd_before = max(nd - HELD, 1)

    def down(g, step, first=True):
        j = step - nd_before if g else step if first else step - nd
        rows = pl.ds(pl.multiple_of(j * dc, 128), dc)
        y = lax.dot_general(hid_rows[g], dw[rows, :], NT_DIMS, preferred_element_type=F32)
        y = (y * wcol[g]).astype(BF)
        for slot in range(slots):
            at = (slot // 2 % B) * 2 + slot // (2 * B)
            dense[step, slot % 2, at * tok : (at + 1) * tok, :] = y[slot * tok : (slot + 1) * tok]
        ccopy(step).start()

    def reduce_steps(step):
        @pl.when((step >= CORE_LAG) & (step < total_steps + CORE_LAG))
        def _():
            j = step - CORE_LAG
            ccopy(j).wait_recv()
            for k in range(B):
                at = pl.ds(k * 2 * tok, 2 * tok)
                s1[j, k] = (dense[j, c, at].astype(F32) + crecv[j, at].astype(F32)).astype(BF)
            for k in range(1, B):
                xcopy(j, k).start()

        @pl.when((step >= X_LAG) & (step < total_steps + X_LAG))
        def _():
            j = step - X_LAG
            pltpu.make_async_copy(xrecv.at[j], xrecv.at[j], xr.at[j]).wait()
            for i in range(2):
                at = pl.ds(i * tok, tok)
                total = s1[j, b, at].astype(F32)
                for k in range(1, B):
                    total += xrecv[j, k - 1, at].astype(F32)
                s2[j, i] = total.astype(BF)
            z1copy(j).start()

        @pl.when((step >= Z_LAG + nd_before) & (step < nd_before + nd + Z_LAG))
        def _():
            j = step - Z_LAG
            z1copy(j).wait_recv()
            s3[j - nd_before] = (s2[j, r].astype(F32) + z1recv[j].astype(F32)).astype(BF)
            z2copy(j - nd_before).start()

    hidden_ready(0)
    weight_ready(2, down_hbm, dw)

    finish = each(hidden, nj, 1)

    @pl.loop(0, nd_before)
    def _(step):
        down(0, step)
        reduce_steps(step)
        for i, item in enumerate(finish):
            pl.when(step == min(1 + i, nd_before - 1))(item)

    hidden_ready(1)

    @pl.loop(nd_before, nd_before + nd)
    def _(step):
        down(1, step)
        reduce_steps(step)

    if nd_before < nd:

        @pl.loop(nd_before + nd, total_steps)
        def _(step):
            down(0, step, False)
            reduce_steps(step)

    @pl.loop(total_steps, total_steps + Z_LAG)
    def _(step):
        reduce_steps(step)

    for j in range(nd):
        near_at = j if j < nd_before else j + nd
        z1copy(near_at).wait_recv()
        z2copy(j).wait_recv()
        total = s2[near_at, r].astype(F32) + z1recv[near_at].astype(F32) + z2recv[j].astype(F32)
        out_ref[:, pl.ds(j * dc, dc)] = total.astype(BF)

    def sent(ref, sem):
        pltpu.make_async_copy(ref, ref, sem).wait()

    sent(G.at[pl.ds(0, (3 + A * (2 * B - 1)) * tok)], gs)
    sent(ysend, ys)
    sent(hid.at[:, :, pl.ds(0, F - FT)], hs)
    sent(crecv, cs)
    sent(xrecv, xs)
    sent(z1recv, z1s)
    sent(z2recv, z2s)


def shards(tokens, routes, route_logits, gate_weight, up_weight, down_weight):
    E = lax.axis_size("expert")
    T = lax.axis_size("tensor")
    tok, D = tokens.shape
    top = routes.shape[1]
    _, Dl, F = gate_weight.shape
    cap = tok // 2
    A = 4
    B = E // (2 * A)
    assert E == A * B * 2 and D == Dl * T
    lanes = -(-2 * E // 128) * 128
    hc = 4 if Dl % (4 * 128) == 0 else 1
    nd = 7 if Dl % (7 * 128) == 0 else 1
    dc = Dl // nd
    FT = F // T
    fc = 256 if FT % 256 == 0 else FT
    nj = FT // fc
    pieces = 4
    NG, RG = 4 * B * tok, 4 * B * cap
    dims = (E, T, A, B, tok, cap, top, Dl, F, lanes, hc, nd, dc, fc, nj, pieces)
    vmem = pl.BlockSpec(memory_space=pltpu.VMEM)
    hbm = pl.BlockSpec(memory_space=pl.ANY)
    dma = pltpu.SemaphoreType.DMA
    return pl.pallas_call(
        functools.partial(kernel, dims),
        out_shape=pltpu.VMEM((tok, Dl), BF),
        in_specs=[hbm] * 6,
        out_specs=vmem,
        scratch_shapes=[
            pltpu.VMEM((top, tok), jnp.int32),
            pltpu.VMEM((top, tok), F32),
            pltpu.VMEM((2 * NG, lanes + Dl), BF),
            pltpu.VMEM((Dl, F), BF),
            pltpu.VMEM((Dl, F), BF),
            pltpu.VMEM((Dl, F), BF),
            pltpu.VMEM((2, RG, Dl), BF),
            pltpu.VMEM((2, NG, RG), BF),
            pltpu.VMEM((2, NG, 1), F32),
            pltpu.VMEM((2, T - 1, nj, 2, RG, fc), BF),
            pltpu.VMEM((2, T - 1, nj, 2, RG, fc), BF),
            pltpu.VMEM((2, nj, 2, RG, fc), F32),
            pltpu.VMEM((T - 1, nj, 2, RG, fc), F32),
            pltpu.VMEM((2, RG, F), BF),
            pltpu.VMEM((2, NG, F), BF),
            pltpu.VMEM((2 * nd, 2, NG // 2, dc), BF),
            pltpu.VMEM((2 * nd, NG // 2, dc), BF),
            pltpu.VMEM((2 * nd, B, 2 * tok, dc), BF),
            pltpu.VMEM((2 * nd, B - 1, 2 * tok, dc), BF),
            pltpu.VMEM((2 * nd, 2, tok, dc), BF),
            pltpu.VMEM((2 * nd, tok, dc), BF),
            pltpu.VMEM((nd, tok, dc), BF),
            pltpu.VMEM((nd, tok, dc), BF),
            dma((2,)),
            dma((3,)),
            dma((hc,)),
            dma,
            dma((3, hc)),
            dma((A, B - 1, hc)),
            dma((B - 1, hc)),
            dma((2, hc)),
            dma,
            dma((2, T - 1, nj)),
            dma,
            dma((2,)),
            dma,
            dma((2 * nd,)),
            dma,
            dma((2 * nd,)),
            dma,
            dma((2 * nd,)),
            dma,
            dma((nd,)),
        ],
        compiler_params=pltpu.CompilerParams(
            collective_id=0, has_side_effects=True, vmem_limit_bytes=60 * 1024 * 1024
        ),
    )(tokens, routes.T, route_logits.T, gate_weight, up_weight, down_weight)


def solution(mesh):
    return jax.shard_map(
        shards,
        mesh=mesh,
        in_specs=(
            P("expert", None),
            P("expert", None),
            P("expert", None),
            P("expert", "tensor", None),
            P("expert", "tensor", None),
            P("expert", "tensor", None),
        ),
        out_specs=P("expert", "tensor"),
        check_vma=False,
    )
```

```python
import functools

import jax
import jax.numpy as jnp
from jax import lax
from jax.experimental import pallas as pl
from jax.experimental.pallas import tpu as pltpu
from jax.sharding import PartitionSpec as P

routed_scale = 2.5
MESH = pl.DeviceIdType.MESH
BF = jnp.bfloat16
F32 = jnp.float32
NT_DIMS = (((1,), (1,)), ((), ()))
CORE_LAG, X_LAG, Z_LAG = 2, 7, 10


def kernel(
    dims,
    tokens_ref,
    routes_hbm,
    logits_hbm,
    gate_hbm,
    up_hbm,
    down_hbm,
    out_ref,
    routes_ref,
    logits_ref,
    G,
    gw,
    uw,
    dw,
    X,
    spread_back,
    wcol,
    ysend,
    yrecv,
    acc,
    kept_part,
    hid,
    hid_rows,
    dense,
    crecv,
    s1,
    xrecv,
    s2,
    z1recv,
    s3,
    z2recv,
    rsem,
    wsem,
    tsem,
    gs,
    gzr,
    gxr,
    gvr,
    gcr,
    ys,
    yr,
    hs,
    hr,
    cs,
    cr,
    xs,
    xr,
    z1s,
    z1r,
    z2s,
    z2r,
):
    E, T, A, B, tok, cap, top, Dl, F, lanes, hc, nd, dc, fc, nj, pieces = dims
    slots = 2 * B * 2
    NG, RG, FT = slots * tok, slots * cap, F // T
    hw = Dl // hc
    e = lax.axis_index("expert")
    t = lax.axis_index("tensor")
    c = lax.rem(e, 2)
    b = lax.rem(e // 2, B)
    a = e // (2 * B)
    r = lax.rem(a, 2)
    half = a // 2
    near = a + 1 - 2 * r
    far = a + 2 - 4 * half
    places = (a, near, far, far + 1 - 2 * r)

    def around(v, i, n):
        return lax.rem(v + i, n)

    def slot_of(ai, bi, ci):
        return (ai * B + bi) * 2 + ci

    def dev(ai, bi, ci):
        return (slot_of(ai, bi, ci), t)

    sibling = dev(a, b, 1 - c)
    z1, z2 = dev(near, b, c), dev(far, b, c)

    barrier = pltpu.get_barrier_semaphore()
    partners = [z1, z2, sibling]
    partners += [dev(a, around(b, k, B), c) for k in range(1, B)]
    partners += [(e, around(t, p, T)) for p in range(1, T)]
    for partner in partners:
        pl.semaphore_signal(barrier, inc=1, device_id=partner, device_id_type=MESH)

    def block(slot):
        return pl.ds(pl.multiple_of(slot * tok, tok), tok)

    route_copies = []
    for which, (src, dst) in enumerate(((routes_hbm, routes_ref), (logits_hbm, logits_ref))):
        copy = pltpu.make_async_copy(src, dst, rsem.at[which])
        copy.start()
        route_copies.append(copy)
    token_copies = []
    for h in range(hc):
        copy = pltpu.make_async_copy(
            tokens_ref.at[:, pl.ds(pl.multiple_of(t * Dl + h * hw, 128), hw)],
            G.at[block(e), pl.ds(lanes + h * hw, hw)],
            tsem.at[h],
        )
        copy.start()
        token_copies.append(copy)

    low_at = lanes // 2
    for copy in route_copies:
        copy.wait()
    scores = jax.nn.sigmoid(logits_ref[...])
    weights = routed_scale * scores / jnp.sum(scores, axis=0, keepdims=True)
    routes = routes_ref[...]
    lane = lax.broadcasted_iota(jnp.int32, (low_at, tok), 0)
    table = jnp.zeros((low_at, tok), F32)
    for k in range(top):
        table += jnp.where(lane == routes[k : k + 1], weights[k : k + 1], 0.0)
    high = table.astype(BF)
    low = (table - high.astype(F32)).astype(BF)
    unit = lax.broadcasted_iota(jnp.int32, (tok, tok), 0) == lax.broadcasted_iota(jnp.int32, (tok, tok), 1)
    unit = jnp.where(unit, 1.0, 0.0).astype(BF)
    both = jnp.concatenate([high, low], axis=0)
    G[block(e), pl.ds(0, lanes)] = lax.dot_general(unit, both, NT_DIMS, preferred_element_type=F32).astype(BF)

    sub = lax.broadcasted_iota(jnp.int32, (NG, NG), 0)
    lan = lax.broadcasted_iota(jnp.int32, (NG, NG), 1)
    same = (sub // tok) == (lan // tok)
    before_row = jnp.where(same & (sub < lan), 1.0, 0.0).astype(BF)
    before_col = jnp.where(same & (lan < sub), 1.0, 0.0).astype(BF)

    pl.semaphore_wait(barrier, len(partners))

    def part(h):
        if isinstance(h, int) and h == 0:
            return pl.ds(0, lanes + hw)
        return pl.ds(pl.multiple_of(lanes + h * hw, 128), hw)

    def gcopy(slot, h, target, sem):
        return pltpu.make_async_remote_copy(
            src_ref=G.at[block(slot), part(h)],
            dst_ref=G.at[block(slot), part(h)],
            send_sem=gs,
            recv_sem=sem,
            device_id=target,
            device_id_type=MESH,
        )

    def gwait(h, sem, count=1):
        span = G.at[pl.ds(0, count * tok), part(h)]
        pltpu.make_async_copy(span, span, sem).wait()

    def by_z(h):
        return h % 2 == 1

    def across(i, h):
        slot = slot_of(places[i], b, c)
        for k in range(1, B) if i < 3 or not by_z(h) else ():
            gcopy(slot, h, dev(a, around(b, k, B), c), gxr.at[i, k - 1, h]).start()
        gcopy(slot, h, sibling, gcr.at[i // 2, h]).start()

    def relay(i, h):
        for k in range(1, B):
            sem = gvr.at[k - 1, h] if i == 3 and by_z(h) else gxr.at[i, k - 1, h]
            slot = slot_of(places[i], around(b, B - k, B), c)
            gwait(h, sem)
            if i == 2 and by_z(h):
                gcopy(slot, h, z1, gvr.at[k - 1, h]).start()
            gcopy(slot, h, sibling, gcr.at[i // 2, h]).start()

    for h in range(hc):
        token_copies[h].wait()
        gcopy(e, h, z1, gzr.at[0, h]).start()
        across(0, h)

    def own_far(h):
        gcopy(e, h, z2, gzr.at[1, h]).start()

    @pl.when(r == half)
    def _():
        for h in range(hc):
            own_far(h)


    step_in = Dl // pieces
    for which, (src, dst) in enumerate(((gate_hbm, gw), (up_hbm, uw), (down_hbm, dw))):
        for p in range(pieces):
            rows = pl.ds(p * step_in, step_in)
            pltpu.make_async_copy(src.at[0, rows], dst.at[rows], wsem.at[which]).start()

    def weight_ready(which, src, dst):
        pltpu.make_async_copy(src.at[0], dst, wsem.at[which]).wait()

    for h in range(hc):
        gwait(h, gzr.at[0, h])
        across(1, h)
        pl.when(r != half)(functools.partial(own_far, h))
        relay(0, h)

    for h in range(hc):
        gwait(h, gzr.at[1, h])
        gcopy(slot_of(far, b, c), h, z1, gzr.at[2, h]).start()
        across(2, h)
        relay(1, h)

    def relay_far(h):
        gwait(h, gzr.at[2, h])
        across(3, h)
        relay(2, h)

    def relay_last(h):
        relay(3, h)

    def group_rows(g):
        return pl.ds(pl.multiple_of((half if g == 0 else 1 - half) * NG, NG), NG)

    def choose(g):
        meta = G[group_rows(g), pl.ds(0, lanes)]
        at = lax.broadcasted_iota(jnp.int32, (8, lanes), 1)
        pick = jnp.where((at == e) | (at == e + low_at), 1.0, 0.0).astype(BF)
        wrow = lax.dot_general(pick, meta, NT_DIMS, preferred_element_type=F32)
        row_on = jnp.where(wrow > 0, 1.0, 0.0)
        row_pos = jnp.dot(row_on.astype(BF), before_row, preferred_element_type=F32)
        row_blk = (lax.broadcasted_iota(jnp.int32, (8, NG), 1) // tok * cap).astype(F32)
        row_at = jnp.where(wrow > 0, row_blk + row_pos, -1.0)[:1]
        slot_row = lax.broadcasted_iota(jnp.int32, (RG, NG), 0).astype(F32)
        S = jnp.where(slot_row == row_at, 1.0, 0.0).astype(BF)

        full = meta.astype(F32)
        at = lax.broadcasted_iota(jnp.int32, (NG, lanes), 1)
        all_on = jnp.where(full > 0, 1.0, 0.0)
        col_pos = jnp.dot(before_col, all_on.astype(BF), preferred_element_type=F32)
        col_blk = (lax.broadcasted_iota(jnp.int32, (NG, lanes), 0) // tok * cap).astype(F32)
        col_at = jnp.where(full > 0, col_blk + col_pos, -1.0)
        col_at = jnp.sum(jnp.where(at == e, col_at, 0.0), axis=1, keepdims=True)
        slot_col = lax.broadcasted_iota(jnp.int32, (NG, RG), 1).astype(F32)
        spread_back[g] = jnp.where(slot_col == col_at, 1.0, 0.0).astype(BF)
        mine = (at == e) | (at == e + low_at)
        wcol[g] = jnp.sum(jnp.where(mine, full, 0.0), axis=1, keepdims=True)
        return S

    chosen = [None, None]

    def collect(g, h):
        gwait(h, gcr.at[g, h], 2 * B)
        if h == 0:
            chosen[g] = choose(g)
        rows = G[group_rows(g), pl.ds(lanes + h * hw, hw)]
        X[g, :, pl.ds(h * hw, hw)] = jnp.dot(chosen[g], rows, preferred_element_type=F32).astype(BF)

    def ycopy(g, p, j):
        return pltpu.make_async_remote_copy(
            src_ref=ysend.at[g, p - 1, j],
            dst_ref=yrecv.at[g, p - 1, j],
            send_sem=ys,
            recv_sem=yr.at[g, p - 1, j],
            device_id=(e, around(t, p, T)),
            device_id_type=MESH,
        )

    def hcols(rank, j):
        return pl.ds(pl.multiple_of(rank * FT + j * fc, 128), fc)

    def hcopy(g, p, j, rank):
        return pltpu.make_async_remote_copy(
            src_ref=hid.at[g, :, hcols(rank, j)],
            dst_ref=hid.at[g, :, hcols(rank, j)],
            send_sem=hs,
            recv_sem=hr.at[g],
            device_id=(e, around(t, p, T)),
            device_id_type=MESH,
        )

    def gate_up_theirs(g, j, first=0, kept=False):
        depth = pl.ds(first, Dl - first)
        for p in range(1, T):
            cols = hcols(around(t, p, T), j)
            for which, w in enumerate((gw, uw)):
                value = jnp.dot(X[g, :, depth], w[depth, cols], preferred_element_type=F32)
                if kept:
                    value += kept_part[p - 1, j, which]
                ysend[g, p - 1, j, which] = value.astype(BF)
            ycopy(g, p, j).start()

    def gate_up_part(g, j, until):
        depth = pl.ds(0, until)
        for p in range(1, T):
            cols = hcols(around(t, p, T), j)
            for which, w in enumerate((gw, uw)):
                kept_part[p - 1, j, which] = jnp.dot(X[g, :, depth], w[depth, cols], preferred_element_type=F32)

    def gate_up_own(g, j):
        cols = hcols(t, j)
        acc[g, j, 0] = jnp.dot(X[g], gw[:, cols], preferred_element_type=F32)
        acc[g, j, 1] = jnp.dot(X[g], uw[:, cols], preferred_element_type=F32)

    def hidden(g, j):
        gv, uv = acc[g, j, 0], acc[g, j, 1]
        for p in range(1, T):
            ycopy(g, p, j).wait_recv()
            gv += yrecv[g, p - 1, j, 0].astype(F32)
            uv += yrecv[g, p - 1, j, 1].astype(F32)
        hid[g, :, hcols(t, j)] = (gv / (1.0 + jnp.exp(-gv)) * uv).astype(BF)
        for p in range(1, T):
            hcopy(g, p, j, t).start()

    def hidden_ready(g):
        span = hid.at[g, :, pl.ds(0, F - FT)]
        pltpu.make_async_copy(span, span, hr.at[g]).wait()
        hid_rows[g] = jnp.dot(spread_back[g], hid[g], preferred_element_type=F32).astype(BF)

    for h in range(hc):
        collect(0, h)
    weight_ready(0, gate_hbm, gw)
    weight_ready(1, up_hbm, uw)
    def run(*items):
        for item in items:
            item()

    def each(fn, n, *lead):
        return [functools.partial(fn, *lead, i) for i in range(n)]

    last, finish = each(relay_last, hc), each(hidden, nj, 0)
    cut = hc // 2
    run(*each(gate_up_theirs, nj, 0))
    run(*each(relay_far, hc))
    run(*each(gate_up_own, nj, 0))
    run(*last[:cut])
    run(*finish[:1])
    run(*last[cut:])
    for h in range(cut):
        collect(1, h)
    run(*finish[1:])
    for j in range(nj if cut else 0):
        gate_up_part(1, j, cut * hw)
    for h in range(cut, hc):
        collect(1, h)
    for j in range(nj):
        gate_up_theirs(1, j, cut * hw, bool(cut))
    run(*each(gate_up_own, nj, 1))

    def ccopy(j):
        return pltpu.make_async_remote_copy(
            src_ref=dense.at[j, 1 - c],
            dst_ref=crecv.at[j],
            send_sem=cs,
            recv_sem=cr.at[j],
            device_id=sibling,
            device_id_type=MESH,
        )

    def xcopy(j, k):
        return pltpu.make_async_remote_copy(
            src_ref=s1.at[j, around(b, k, B)],
            dst_ref=xrecv.at[j, k - 1],
            send_sem=xs,
            recv_sem=xr.at[j],
            device_id=dev(a, around(b, k, B), c),
            device_id_type=MESH,
        )

    def z1copy(j):
        return pltpu.make_async_remote_copy(
            src_ref=s2.at[j, 1 - r],
            dst_ref=z1recv.at[j],
            send_sem=z1s,
            recv_sem=z1r.at[j],
            device_id=z1,
            device_id_type=MESH,
        )

    def z2copy(j):
        return pltpu.make_async_remote_copy(
            src_ref=s3.at[j],
            dst_ref=z2recv.at[j],
            send_sem=z2s,
            recv_sem=z2r.at[j],
            device_id=z2,
            device_id_type=MESH,
        )

    total_steps = 2 * nd

    def down(g, step):
        j = step - g * nd
        rows = pl.ds(pl.multiple_of(j * dc, 128), dc)
        y = lax.dot_general(hid_rows[g], dw[rows, :], NT_DIMS, preferred_element_type=F32)
        y = (y * wcol[g]).astype(BF)
        for slot in range(slots):
            at = (slot // 2 % B) * 2 + slot // (2 * B)
            dense[step, slot % 2, at * tok : (at + 1) * tok, :] = y[slot * tok : (slot + 1) * tok]

    def core_add(j):
        for k in range(B):
            at = pl.ds(k * 2 * tok, 2 * tok)
            s1[j, k] = (dense[j, c, at].astype(F32) + crecv[j, at].astype(F32)).astype(BF)

    def x_send(j):
        for k in range(1, B):
            xcopy(j, k).start()

    def x_wait(j):
        pltpu.make_async_copy(xrecv.at[j], xrecv.at[j], xr.at[j]).wait()

    def x_add(j):
        for i in range(2):
            at = pl.ds(i * tok, tok)
            total = s1[j, b, at].astype(F32)
            for k in range(1, B):
                total += xrecv[j, k - 1, at].astype(F32)
            s2[j, i] = total.astype(BF)

    def reduce_steps(step):
        @pl.when((step >= CORE_LAG) & (step < total_steps + CORE_LAG))
        def _():
            j = step - CORE_LAG
            ccopy(j).wait_recv()
            core_add(j)
            x_send(j)

        @pl.when((step >= X_LAG) & (step < total_steps + X_LAG))
        def _():
            j = step - X_LAG
            x_wait(j)
            x_add(j)
            z1copy(j).start()

        @pl.when((step >= Z_LAG + nd) & (step < nd + nd + Z_LAG))
        def _():
            j = step - Z_LAG
            z1copy(j).wait_recv()
            s3[j - nd] = (s2[j, r].astype(F32) + z1recv[j].astype(F32)).astype(BF)
            z2copy(j - nd).start()

    hidden_ready(0)
    weight_ready(2, down_hbm, dw)

    finish = each(hidden, nj, 1)

    @pl.loop(0, nd)
    def _(step):
        down(0, step)
        ccopy(step).start()
        reduce_steps(step)
        for i, item in enumerate(finish):
            pl.when(step == min(1 + i, nd - 1))(item)

    hidden_ready(1)

    steady = X_LAG <= nd <= Z_LAG

    @pl.loop(nd, total_steps)
    def _(step):
        if steady:
            jc, jx = step - CORE_LAG, step - X_LAG
            ccopy(jc).wait_recv()
            x_wait(jx)
            core_add(jc)
            x_add(jx)
            down(1, step)
            ccopy(step).start()
            x_send(jc)
            z1copy(jx).start()
        else:
            down(1, step)
            ccopy(step).start()
            reduce_steps(step)

    @pl.loop(total_steps, total_steps + Z_LAG)
    def _(step):
        reduce_steps(step)

    for j in range(nd):
        z1copy(j).wait_recv()
        z2copy(j).wait_recv()
        total = s2[j, r].astype(F32) + z1recv[j].astype(F32) + z2recv[j].astype(F32)
        out_ref[:, pl.ds(j * dc, dc)] = total.astype(BF)

    def sent(ref, sem):
        pltpu.make_async_copy(ref, ref, sem).wait()

    sent(G.at[pl.ds(0, (3 + A * (2 * B - 1)) * tok)], gs)
    sent(ysend, ys)
    sent(hid.at[:, :, pl.ds(0, F - FT)], hs)
    sent(crecv, cs)
    sent(xrecv, xs)
    sent(z1recv, z1s)
    sent(z2recv, z2s)


def shards(tokens, routes, route_logits, gate_weight, up_weight, down_weight):
    E = lax.axis_size("expert")
    T = lax.axis_size("tensor")
    tok, D = tokens.shape
    top = routes.shape[1]
    _, Dl, F = gate_weight.shape
    cap = tok // 2
    A = 4
    B = E // (2 * A)
    assert E == A * B * 2 and D == Dl * T
    lanes = -(-2 * E // 128) * 128
    hc = 4 if Dl % (4 * 128) == 0 else 1
    nd = 7 if Dl % (7 * 128) == 0 else 1
    dc = Dl // nd
    FT = F // T
    fc = 256 if FT % 256 == 0 else FT
    nj = FT // fc
    pieces = 4
    NG, RG = 4 * B * tok, 4 * B * cap
    dims = (E, T, A, B, tok, cap, top, Dl, F, lanes, hc, nd, dc, fc, nj, pieces)
    vmem = pl.BlockSpec(memory_space=pltpu.VMEM)
    hbm = pl.BlockSpec(memory_space=pl.ANY)
    dma = pltpu.SemaphoreType.DMA
    return pl.pallas_call(
        functools.partial(kernel, dims),
        out_shape=pltpu.VMEM((tok, Dl), BF),
        in_specs=[hbm] * 6,
        out_specs=vmem,
        scratch_shapes=[
            pltpu.VMEM((top, tok), jnp.int32),
            pltpu.VMEM((top, tok), F32),
            pltpu.VMEM((2 * NG, lanes + Dl), BF),
            pltpu.VMEM((Dl, F), BF),
            pltpu.VMEM((Dl, F), BF),
            pltpu.VMEM((Dl, F), BF),
            pltpu.VMEM((2, RG, Dl), BF),
            pltpu.VMEM((2, NG, RG), BF),
            pltpu.VMEM((2, NG, 1), F32),
            pltpu.VMEM((2, T - 1, nj, 2, RG, fc), BF),
            pltpu.VMEM((2, T - 1, nj, 2, RG, fc), BF),
            pltpu.VMEM((2, nj, 2, RG, fc), F32),
            pltpu.VMEM((T - 1, nj, 2, RG, fc), F32),
            pltpu.VMEM((2, RG, F), BF),
            pltpu.VMEM((2, NG, F), BF),
            pltpu.VMEM((2 * nd, 2, NG // 2, dc), BF),
            pltpu.VMEM((2 * nd, NG // 2, dc), BF),
            pltpu.VMEM((2 * nd, B, 2 * tok, dc), BF),
            pltpu.VMEM((2 * nd, B - 1, 2 * tok, dc), BF),
            pltpu.VMEM((2 * nd, 2, tok, dc), BF),
            pltpu.VMEM((2 * nd, tok, dc), BF),
            pltpu.VMEM((nd, tok, dc), BF),
            pltpu.VMEM((nd, tok, dc), BF),
            dma((2,)),
            dma((3,)),
            dma((hc,)),
            dma,
            dma((3, hc)),
            dma((A, B - 1, hc)),
            dma((B - 1, hc)),
            dma((2, hc)),
            dma,
            dma((2, T - 1, nj)),
            dma,
            dma((2,)),
            dma,
            dma((2 * nd,)),
            dma,
            dma((2 * nd,)),
            dma,
            dma((2 * nd,)),
            dma,
            dma((nd,)),
        ],
        compiler_params=pltpu.CompilerParams(
            collective_id=0, has_side_effects=True, vmem_limit_bytes=60 * 1024 * 1024
        ),
    )(tokens, routes.T, route_logits.T, gate_weight, up_weight, down_weight)


def solution(mesh):
    return jax.shard_map(
        shards,
        mesh=mesh,
        in_specs=(
            P("expert", None),
            P("expert", None),
            P("expert", None),
            P("expert", "tensor", None),
            P("expert", "tensor", None),
            P("expert", "tensor", None),
        ),
        out_specs=P("expert", "tensor"),
        check_vma=False,
    )
```
